32 devices in a mesh: seq: 8 (over z, y), mp: 4 (over x, core).
Axes of the slice: x: 2, y: 2, z: 4, core: 2. Of those that a mesh axis runs over, the one named last changes fastest.
Arguments:
- hidden_in: bfloat16 [2, 1024, 2048], P(None, 'seq'), may hold values from -6 to 6
- attn_gain: float32 [2048], replicated, may hold values from 0.1 to 1.9
- q_weight: bfloat16 [2048, 2048], P(None, 'mp'), may hold values from -0.125 to 0.125
- q_bias: float32 [2048], P('mp'), may hold values from -60 to 60
- k_weight: bfloat16 [2048, 256], replicated, may hold values from -0.125 to 0.125
- k_bias: float32 [256], replicated, may hold values from -60 to 60
- v_weight: bfloat16 [2048, 256], replicated, may hold values from -0.125 to 0.125
- v_bias: float32 [256], replicated, may hold values from -3 to 3
- o_weight: bfloat16 [2048, 2048], P('mp'), may hold values from -0.125 to 0.125
- mlp_gain: float32 [2048], replicated, may hold values from 0.1 to 1.9
- gate_weight: bfloat16 [2048, 5632], P('seq', 'mp'), may hold values from -0.125 to 0.125
- up_weight: bfloat16 [2048, 5632], P('seq', 'mp'), may hold values from -0.125 to 0.125
- down_weight: bfloat16 [2048, 5632], P('seq', 'mp'), may hold values from -0.078125 to 0.078125
- lengths: int32 [2], replicated, may hold values from 512 to 1024
Outputs:
- layer_out: bfloat16 [2, 1024, 2048], P(None, 'seq', 'mp')
- influence: float32 [2, 1024], P(None, 'seq')
- score: float32 [2], replicated
The draws below stay inside these ranges and needn't reach their ends.
Inputs may be any that keep to these rules, and one draw needn't show every extreme that they name: `lengths`: tokens at positions 512 and later may be invalid.
All inputs are finite; a program needn't handle non-finite values.
Results may differ from the reference program's by a relative error of at most 0.02.
The reference program's roundings to bfloat16 on the way (of `normed`, `attn`, `residual`, `mlp_in` and `activated`) count: a program that leaves them out, or rounds other values in their place, can miss the bound.
Values may be sent and summed in bfloat16 or wider, within the bound.
A program may use at most 192 MiB of HBM per device.

```python
import jax
import jax.numpy as jnp
from jax import lax

D = 2048
HEADS = 16
KV_HEADS = 2
HEAD = 128
FF = 5632
SEQS = 2
SEQ_LEN = 1024
N_MP = 4


def draw_q_bias(key, part):
    noise = jax.random.normal(jax.random.fold_in(key, 11), (HEADS * HEAD,), jnp.float32)
    return jnp.clip(noise * 0.5, -3.0, 3.0)


def draw_k_bias(key, part):
    noise = jax.random.normal(jax.random.fold_in(key, 12), (KV_HEADS * HEAD,), jnp.float32)
    return jnp.clip(noise * 0.5, -3.0, 3.0)


def shard_levels(stream_key, dims, shards, low, top_value):
    factor_of, own = 1.0, jax.random.fold_in(stream_key, 6)
    for axis_at, parts in shards:
        steps = jnp.exp(jax.random.uniform(jax.random.fold_in(own, axis_at), (parts,), jnp.float32, low / len(shards), top_value / len(shards)))
        factor_of = factor_of * jnp.repeat(steps, dims[axis_at] // parts).reshape([-1 if axis == axis_at else 1 for axis in range(len(dims))])
    return factor_of


def centred(key, shape, scale, most, cuts=(), held_as=jnp.bfloat16):
    drawn = scale * jax.random.normal(key, shape, jnp.float32)
    if cuts:
        drawn = drawn * shard_levels(key, shape, cuts, -0.22, 0.18)
    return jnp.clip(drawn, -most, most).astype(held_as)


def setup_inputs(seed: int = 0) -> dict:
    seeds = jax.random.split(jax.random.key(seed), 15)
    return {
        "hidden_in": centred(seeds[0], (SEQS, SEQ_LEN, D), 1.0, 6.0, ((1, 8),)),
        "attn_gain": jnp.clip(1.0 + 0.18 * jax.random.normal(seeds[1], (D,), jnp.float32), 0.1, 1.9),
        "q_weight": centred(seeds[2], (D, HEADS * HEAD), D ** -0.5, 0.125, ((1, 4),)),
        "q_bias": draw_q_bias(jax.random.fold_in(seeds[14], 71), 0),
        "k_weight": centred(seeds[4], (D, KV_HEADS * HEAD), D ** -0.5, 0.125),
        "k_bias": draw_k_bias(jax.random.fold_in(seeds[14], 71), 0),
        "v_weight": centred(seeds[6], (D, KV_HEADS * HEAD), D ** -0.5, 0.125),
        "v_bias": centred(seeds[7], (KV_HEADS * HEAD,), 0.5, 3.0, (), jnp.float32),
        "o_weight": centred(seeds[8], (HEADS * HEAD, D), (HEADS * HEAD) ** -0.5, 0.125, ((0, 4),)),
        "mlp_gain": jnp.clip(1.0 + 0.18 * jax.random.normal(seeds[9], (D,), jnp.float32), 0.1, 1.9),
        "gate_weight": centred(seeds[10], (D, FF), D ** -0.5, 0.125, ((0, 8), (1, 4))),
        "up_weight": centred(seeds[11], (D, FF), D ** -0.5, 0.125, ((0, 8), (1, 4))),
        "down_weight": centred(seeds[12], (D, FF), FF ** -0.5, 0.078125, ((0, 8), (1, 4))),
        "lengths": jax.random.randint(seeds[13], (SEQS,), SEQ_LEN // 2, SEQ_LEN + 1).astype(jnp.int32),
    }


rope_base = 1000000.0
norm_eps = 1e-06
masked_score = -1e+30

def rms_scale(values, gain):
    widened = values.astype(jnp.float32)
    factor = lax.rsqrt(lax.optimization_barrier(jnp.mean(widened * widened, axis=-1, keepdims=True)) + norm_eps)
    return (widened * factor * gain.astype(jnp.float32)).astype(jnp.bfloat16)

def rotate(values, positions):
    head_width = values.shape[-1]
    half_width = head_width // 2
    inv_freq = rope_base ** (-(jnp.arange(half_width, dtype=jnp.float32) * 2.0) / head_width)
    angles = positions.astype(jnp.float32)[:, None] * inv_freq[None, :]
    angles = jnp.concatenate([angles, angles], axis=-1)
    first_part = values[..., :half_width]
    second_part = values[..., half_width:]
    turned = jnp.concatenate([-second_part, first_part], axis=-1)
    return values * jnp.cos(angles) + turned * jnp.sin(angles)

def round_trip(values):
    return lax.optimization_barrier(values.astype(jnp.bfloat16)).astype(jnp.float32)

def reference(hidden_in, attn_gain, q_weight, q_bias, k_weight, k_bias, v_weight, v_bias, o_weight, mlp_gain, gate_weight, up_weight, down_weight, lengths):
    seqs_n, seq_len, width = hidden_in.shape
    flat_in = hidden_in.reshape(seqs_n * seq_len, width)
    normed = rms_scale(flat_in, attn_gain)
    query_all = jnp.dot(normed, q_weight, preferred_element_type=jnp.float32) + q_bias
    key_all = jnp.dot(normed, k_weight, preferred_element_type=jnp.float32) + k_bias
    value_all = (jnp.dot(normed, v_weight, preferred_element_type=jnp.float32) + v_bias).astype(jnp.bfloat16)
    positions = jnp.arange(seq_len, dtype=jnp.int32)
    queries = rotate(query_all.reshape(seqs_n, seq_len, HEADS, HEAD).transpose(0, 2, 1, 3), positions).astype(jnp.bfloat16)
    keys = rotate(key_all.reshape(seqs_n, seq_len, KV_HEADS, HEAD).transpose(0, 2, 1, 3), positions).astype(jnp.bfloat16)
    values = value_all.reshape(seqs_n, seq_len, KV_HEADS, HEAD).transpose(0, 2, 1, 3)
    group_size = HEADS // KV_HEADS
    score_scale = HEAD ** (-0.5)
    allowed = positions[None, :] <= positions[:, None]

    def one_head(index):
        seq_index = index // HEADS
        head_index = index % HEADS
        query_rows = queries[seq_index, head_index]
        key_rows = keys[seq_index, head_index // group_size]
        value_rows = values[seq_index, head_index // group_size]
        scores = jnp.dot(query_rows, key_rows.T, preferred_element_type=jnp.float32) * score_scale
        scores = jnp.where(allowed, scores, masked_score)
        top_score = lax.optimization_barrier(jnp.max(scores, axis=-1, keepdims=True))
        weights = jnp.where(allowed, jnp.exp(scores - top_score), 0.0)
        totals = lax.optimization_barrier(jnp.sum(weights, axis=-1, keepdims=True))
        mixed = jnp.dot(weights.astype(jnp.bfloat16), value_rows, preferred_element_type=jnp.float32)
        return (mixed / totals).astype(jnp.bfloat16)
    attn = lax.map(one_head, jnp.arange(seqs_n * HEADS, dtype=jnp.int32))
    attn = attn.reshape(seqs_n, HEADS, seq_len, HEAD).transpose(0, 2, 1, 3).reshape(seqs_n * seq_len, HEADS * HEAD)
    group_cols = HEADS // N_MP * HEAD
    attn_out = jnp.zeros((seqs_n * seq_len, width), jnp.float32)
    for group in range(N_MP):
        partial_out = jnp.dot(attn[:, group * group_cols:(group + 1) * group_cols], o_weight[group * group_cols:(group + 1) * group_cols], preferred_element_type=jnp.float32)
        attn_out = attn_out + round_trip(partial_out)
    residual = (flat_in.astype(jnp.float32) + attn_out).astype(jnp.bfloat16)
    mlp_in = rms_scale(residual, mlp_gain)
    gate_sum = jnp.dot(mlp_in, gate_weight, preferred_element_type=jnp.float32)
    up_sum = jnp.dot(mlp_in, up_weight, preferred_element_type=jnp.float32)
    activated = (jax.nn.silu(gate_sum) * up_sum).astype(jnp.bfloat16)
    ff_cols = FF // N_MP
    mlp_out = jnp.zeros((seqs_n * seq_len, width), jnp.float32)
    for group in range(N_MP):
        partial_out = jnp.dot(activated[:, group * ff_cols:(group + 1) * ff_cols], down_weight[:, group * ff_cols:(group + 1) * ff_cols].T, preferred_element_type=jnp.float32)
        mlp_out = mlp_out + round_trip(partial_out)
    layer_out = (residual.astype(jnp.float32) + mlp_out).astype(jnp.bfloat16)
    in_wide = flat_in.astype(jnp.float32)
    out_wide = layer_out.astype(jnp.float32)
    cross = lax.optimization_barrier(jnp.sum(in_wide * out_wide, axis=-1)).reshape(seqs_n, seq_len)
    in_norm = lax.optimization_barrier(jnp.sum(in_wide * in_wide, axis=-1)).reshape(seqs_n, seq_len)
    out_norm = lax.optimization_barrier(jnp.sum(out_wide * out_wide, axis=-1)).reshape(seqs_n, seq_len)
    cosine = cross / jnp.sqrt((in_norm + norm_eps) * (out_norm + norm_eps))
    valid = positions[None, :] < lengths[:, None]
    influence = jnp.where(valid, 1.0 - cosine, 0.0)
    score = lax.optimization_barrier(jnp.sum(influence, axis=1)) / lengths.astype(jnp.float32)
    return (layer_out.reshape(seqs_n, seq_len, width), influence, score)
```

```python
import functools

import jax
import jax.numpy as jnp
from jax import lax
from jax.experimental import pallas as pl
from jax.experimental.pallas import tpu as pltpu
from jax.sharding import PartitionSpec as P

HEADS = 16
KV_HEADS = 2
HEAD = 128


rope_base = 1000000.0
norm_eps = 1e-06
masked_score = -1e30


def rms_scale(values, gain):
    widened = values.astype(jnp.float32)
    factor = lax.rsqrt(jnp.mean(widened * widened, axis=-1, keepdims=True) + norm_eps)
    return (widened * factor * gain).astype(jnp.bfloat16)


def rotate(values, positions):
    head_width = values.shape[-1]
    half_width = head_width // 2
    inv_freq = rope_base ** (-(jnp.arange(half_width, dtype=jnp.float32) * 2.0) / head_width)
    angles = positions.astype(jnp.float32)[:, None] * inv_freq[None, :]
    angles = jnp.concatenate([angles, angles], axis=-1)
    first_part = values[..., :half_width]
    second_part = values[..., half_width:]
    turned = jnp.concatenate([-second_part, first_part], axis=-1)
    return values * jnp.cos(angles) + turned * jnp.sin(angles)


def attend_update(state, queries, first_pos, key_piece, value_piece):
    run_max, run_sum, run_acc = state
    score_scale = queries.shape[-1] ** (-0.5)
    query_pos = first_pos + jnp.arange(queries.shape[2], dtype=jnp.int32)
    key_pos = jnp.arange(key_piece.shape[1], dtype=jnp.int32)
    scores = (
        jnp.einsum("shqd,skd->shqk", queries, key_piece, preferred_element_type=jnp.float32)
        * score_scale
    )
    allowed = key_pos[None, :] <= query_pos[:, None]
    scores = jnp.where(allowed, scores, masked_score)
    new_max = jnp.maximum(run_max, jnp.max(scores, axis=-1))
    weights = jnp.where(allowed, jnp.exp(scores - new_max[..., None]), 0.0)
    new_sum = jnp.sum(weights, axis=-1)
    mixed = jnp.einsum(
        "shqk,skd->shqd",
        weights.astype(jnp.bfloat16),
        value_piece,
        preferred_element_type=jnp.float32,
    )
    return (new_max, new_sum, mixed)


def local(
    hidden_in,
    attn_gain,
    q_weight,
    q_bias,
    k_weight,
    k_bias,
    v_weight,
    v_bias,
    o_weight,
    mlp_gain,
    gate_weight,
    up_weight,
    down_weight,
    lengths,
):
    seqs_n, tok_n, width = hidden_in.shape
    seq_rank = lax.axis_index("seq")
    mp_devices = lax.axis_size("mp")
    mp_rank = lax.axis_index("mp")
    heads_here = q_weight.shape[1] // HEAD
    group_size = HEADS // KV_HEADS
    kv_index = mp_rank * heads_here // group_size
    flat_in = hidden_in.reshape(seqs_n * tok_n, width)
    normed = rms_scale(flat_in, attn_gain)
    query_all = jnp.dot(normed, q_weight, preferred_element_type=jnp.float32) + q_bias
    key_cols = lax.dynamic_slice_in_dim(k_weight, kv_index * HEAD, HEAD, 1)
    value_cols = lax.dynamic_slice_in_dim(v_weight, kv_index * HEAD, HEAD, 1)
    key_shift = lax.dynamic_slice_in_dim(k_bias, kv_index * HEAD, HEAD, 0)
    value_shift = lax.dynamic_slice_in_dim(v_bias, kv_index * HEAD, HEAD, 0)
    key_all = jnp.dot(normed, key_cols, preferred_element_type=jnp.float32) + key_shift
    value_rows = (
        jnp.dot(normed, value_cols, preferred_element_type=jnp.float32) + value_shift
    ).astype(jnp.bfloat16)
    positions = seq_rank * tok_n + jnp.arange(tok_n, dtype=jnp.int32)
    rotated_q = rotate(
        query_all.reshape(seqs_n, tok_n, heads_here, HEAD).transpose(0, 2, 1, 3), positions
    ).astype(jnp.bfloat16)
    rotated_k = rotate(key_all.reshape(seqs_n, tok_n, HEAD), positions).astype(jnp.bfloat16)
    value_rows = value_rows.reshape(seqs_n, tok_n, HEAD)
    query_sets = ((rotated_q, seq_rank * tok_n),)
    initial = tuple(
        (
            (
                jnp.full(entry[0].shape[:3], masked_score, jnp.float32),
                jnp.zeros(entry[0].shape[:3], jnp.float32),
                jnp.zeros(entry[0].shape, jnp.float32),
            )
            for entry in query_sets
        )
    )
    key_start = jnp.int32(0)
    key_piece = lax.all_gather(rotated_k, "seq", axis=1, tiled=True)
    value_piece = lax.all_gather(value_rows, "seq", axis=1, tiled=True)
    updated = []
    for state, query_entry in zip(initial, query_sets):
        queries, first_pos = query_entry
        last_pos = first_pos + queries.shape[2] - 1

        def run_update(current):
            return attend_update(current, queries, first_pos, key_piece, value_piece)

        def keep_state(current):
            return current

        updated.append(lax.cond(key_start <= last_pos, run_update, keep_state, state))
    results = tuple(updated)
    finished = [(entry[2] / entry[1][..., None]).astype(jnp.bfloat16) for entry in results]
    attn = finished[0]
    attn = attn.transpose(0, 2, 1, 3).reshape(seqs_n * tok_n, heads_here * HEAD)
    projected = jnp.dot(attn, o_weight, preferred_element_type=jnp.float32)
    quarter = width // mp_devices
    own_in = lax.dynamic_slice_in_dim(flat_in, mp_rank * quarter, quarter, 1)
    summed = lax.psum(projected.astype(jnp.bfloat16), "mp").astype(jnp.float32)
    residual = (flat_in.astype(jnp.float32) + summed).astype(jnp.bfloat16)
    resid_part = lax.dynamic_slice_in_dim(residual, mp_rank * quarter, quarter, 1)
    mlp_in = rms_scale(residual, mlp_gain)
    gate_sum = jnp.dot(
        mlp_in,
        lax.all_gather(gate_weight, "seq", axis=0, tiled=True),
        preferred_element_type=jnp.float32,
    )
    up_sum = jnp.dot(
        mlp_in,
        lax.all_gather(up_weight, "seq", axis=0, tiled=True),
        preferred_element_type=jnp.float32,
    )
    activated = (jax.nn.silu(gate_sum) * up_sum).astype(jnp.bfloat16)
    down_part = lax.dot_general(
        activated,
        lax.all_gather(down_weight, "seq", axis=0, tiled=True),
        (((1,), (1,)), ((), ())),
        preferred_element_type=jnp.float32,
    )
    mlp_share = lax.psum_scatter(
        down_part.astype(jnp.bfloat16), "mp", scatter_dimension=1, tiled=True
    ).astype(jnp.float32)
    layer_part = (resid_part.astype(jnp.float32) + mlp_share).astype(jnp.bfloat16)
    in_share = own_in.astype(jnp.float32)
    out_share = layer_part.astype(jnp.float32)
    cross_part = jnp.sum(in_share * out_share, axis=-1).reshape(seqs_n, tok_n)
    out_part = jnp.sum(out_share * out_share, axis=-1).reshape(seqs_n, tok_n)
    cross, out_norm = lax.psum((cross_part, out_part), "mp")
    in_wide = flat_in.astype(jnp.float32)
    in_norm = jnp.sum(in_wide * in_wide, axis=-1).reshape(seqs_n, tok_n)
    cosine = cross / jnp.sqrt((in_norm + norm_eps) * (out_norm + norm_eps))
    valid = positions[None, :] < lengths[:, None]
    influence = jnp.where(valid, 1.0 - cosine, 0.0)
    seq_total = lax.psum(jnp.sum(influence, axis=1), "seq")
    score = seq_total / lengths.astype(jnp.float32)
    return (layer_part.reshape(seqs_n, tok_n, quarter), influence, score)


MESH = pl.DeviceIdType.MESH
PAIR = 2
VMEM_BYTES = 60 * 1024 * 1024


def layer_kernel(
    n,
    m,
    q_ref,
    kv_ref,
    w_ref,
    o_ref,
    h_ref,
    g_ref,
    out_ref,
    kv_all,
    w_all,
    attn,
    part,
    rs_buf,
    resid,
    mlp_in,
    sums,
    c_buf,
    b_buf,
    a_buf,
    z_buf,
    kv_send,
    kv_recv,
    fw_send,
    fw_recv,
    w_send,
    w_recv,
    rs_send,
    rs_recv,
    zg_send,
    ag_send,
    ag_recv,
    c_send,
    c_recv,
    b_send,
    b_recv,
    a_send,
    a_recv,
    zs_send,
    zs_recv,
):
    f32, bf16 = jnp.float32, jnp.bfloat16
    s = lax.axis_index("seq")
    mp = lax.axis_index("mp")
    nz = n // PAIR
    nx = m // PAIR
    z, y = s // PAIR, s % PAIR
    x, c = mp // PAIR, mp % PAIR
    tok, width_q = h_ref.shape
    seqs_n, heads_here, tok_n, head_w = q_ref.shape
    rows = w_ref.shape[3]

    def seq_of(zz, yy):
        return zz * PAIR + yy

    def mp_of(xx, cc):
        return xx * PAIR + cc

    ya, xa = y + (1 - c) * (1 - 2 * y), x + c * (1 - 2 * x)
    yb, xb = y + c * (1 - 2 * y), x + (1 - c) * (1 - 2 * x)
    dev_a = (seq_of(z, ya), mp_of(xa, c))
    dev_b = (seq_of(z, yb), mp_of(xb, c))
    dev_c = (s, mp_of(x, 1 - c))

    def remote(source, target, sent, arrived, device):
        return pltpu.make_async_remote_copy(
            src_ref=source,
            dst_ref=target,
            send_sem=sent,
            recv_sem=arrived,
            device_id=device,
            device_id_type=MESH,
        )

    barrier = pltpu.get_barrier_semaphore()
    for d in range(1, n):
        pl.semaphore_signal(barrier, inc=1, device_id=((s + d) % n, mp), device_id_type=MESH)
    for d in range(1, m):
        pl.semaphore_signal(barrier, inc=1, device_id=(s, (mp + d) % m), device_id_type=MESH)
    pl.semaphore_wait(barrier, n - 1 + m - 1)

    def kv_copy(d):
        return remote(
            kv_ref.at[c], kv_all.at[c, s], kv_send.at[d], kv_recv.at[s], ((s + d) % n, mp)
        )

    def w_copy(d):
        peer = (s + d) % n
        here = pl.ds(pl.multiple_of(s * rows, rows), rows)
        return remote(
            w_ref.at[:, peer], w_all.at[:, :, here], w_send.at[d], w_recv.at[s], (peer, mp)
        )

    for d in range(1, n):
        @pl.when((s + d) % n > s)
        def _():
            kv_copy(d).start()

    for d in range(1, n):
        w_copy(d).start()

    kv_all[0, s] = kv_ref[0]
    kv_all[1, s] = kv_ref[1]
    w_all[:, :, pl.ds(pl.multiple_of(s * rows, rows), rows)] = w_ref[:, s]
    for j in range(n):
        @pl.when(j > s)
        def _():
            kv_all[0, j] = jnp.zeros_like(kv_ref[0])
            kv_all[1, j] = jnp.zeros_like(kv_ref[1])

    def fw_copy(j, cc):
        return remote(kv_all.at[cc, j], kv_all.at[cc, j], fw_send.at[j], fw_recv.at[j], dev_c)

    for j in range(n):
        @pl.when(j < s)
        def _():
            remote(kv_ref.at[c], kv_all.at[c, j], kv_send.at[0], kv_recv.at[j], dev_c).wait_recv()
            fw_copy(j, c).start()

    for j in range(n):
        @pl.when(j < s)
        def _():
            fw_copy(j, 1 - c).wait_recv()

    scale = head_w ** (-0.5)
    query_pos = s * tok_n + lax.broadcasted_iota(jnp.int32, (tok_n, n * tok_n), 0)
    key_pos = lax.broadcasted_iota(jnp.int32, (tok_n, n * tok_n), 1)
    allowed = key_pos <= query_pos
    for i in range(seqs_n):
        keys = kv_all[0, :, i].reshape(n * tok_n, head_w)
        vals = kv_all[1, :, i].reshape(n * tok_n, head_w)
        for h in range(heads_here):
            scores = lax.dot_general(
                q_ref[i, h], keys, (((1,), (1,)), ((), ())), preferred_element_type=f32
            )
            scores = jnp.where(allowed, scores * scale, masked_score)
            top = jnp.max(scores, axis=-1, keepdims=True)
            weights = jnp.where(allowed, jnp.exp(scores - top), 0.0)
            total = jnp.sum(weights, axis=-1, keepdims=True)
            mixed = jnp.dot(weights.astype(bf16), vals, preferred_element_type=f32)
            attn[i * tok_n : (i + 1) * tok_n, h * head_w : (h + 1) * head_w] = (
                mixed / total
            ).astype(bf16)

    for e in range(m):
        part[e] = jnp.dot(
            attn[...], o_ref[:, e * width_q : (e + 1) * width_q], preferred_element_type=f32
        ).astype(bf16)

    def rs_copy(e):
        peer = (mp + e) % m
        return remote(part.at[peer], rs_buf.at[mp], rs_send.at[e], rs_recv.at[mp], (s, peer))

    for e in range(1, m):
        rs_copy(e).start()
    summed = part[mp].astype(f32)
    for e in range(1, m):
        peer = (mp + e) % m
        remote(
            part.at[peer], rs_buf.at[peer], rs_send.at[e], rs_recv.at[peer], (s, peer)
        ).wait_recv()
        summed = summed + rs_buf[peer].astype(f32)
    resid[s, mp] = (h_ref[...].astype(f32) + summed).astype(bf16)

    def ag_copy(kind, bs, bm, device):
        return remote(
            resid.at[bs, bm], resid.at[bs, bm], ag_send.at[kind, bs, bm], ag_recv.at[bs, bm], device
        )

    def ag_wait(bs, bm):
        ag_copy(0, bs, bm, dev_c).wait_recv()

    def z_copy(dz):
        return remote(
            resid.at[s, mp],
            resid.at[s, mp],
            zg_send.at[dz],
            ag_recv.at[s, mp],
            (seq_of((z + dz) % nz, y), mp),
        )

    for dz in range(1, nz):
        z_copy(dz).start()
    for dz in range(nz):
        bs, bm = seq_of((z + dz) % nz, y), mp
        if dz:
            ag_wait(bs, bm)
        ag_copy(0, bs, bm, dev_a).start()
        ag_copy(1, bs, bm, dev_b).start()
        ag_copy(2, bs, bm, dev_c).start()
    for dz in range(nz):
        bs, bm = seq_of((z + dz) % nz, ya), mp_of(xa, c)
        ag_wait(bs, bm)
        ag_copy(1, bs, bm, dev_b).start()
        ag_copy(2, bs, bm, dev_c).start()
    for dz in range(nz):
        for yy, xx in ((yb, xb), (1 - y, 1 - x)):
            bs, bm = seq_of((z + dz) % nz, yy), mp_of(xx, c)
            ag_wait(bs, bm)
            ag_copy(2, bs, bm, dev_c).start()

    for d in range(1, n):
        peer = (s + d) % n
        here = pl.ds(pl.multiple_of(peer * rows, rows), rows)
        remote(
            w_ref.at[:, peer], w_all.at[:, :, here], w_send.at[d], w_recv.at[peer], (peer, mp)
        ).wait_recv()

    def c_copy(t, xx):
        return remote(
            sums.at[t, mp_of(xx, 1 - c)],
            c_buf.at[t, xx],
            c_send.at[t, xx],
            c_recv.at[t, xx],
            dev_c,
        )

    def chunk(t, carry):
        for xx in range(nx):
            ag_wait(t, mp_of(xx, 1 - c))
        total = jnp.zeros((tok, 1), f32)
        for e in range(m):
            piece = resid[t, e].astype(f32)
            total = total + jnp.sum(piece * piece, axis=-1, keepdims=True)
        factor = lax.rsqrt(total / (m * width_q) + norm_eps)
        for e in range(m):
            cols = slice(e * width_q, (e + 1) * width_q)
            mlp_in[:, cols] = (resid[t, e].astype(f32) * factor * g_ref[:, cols]).astype(bf16)
        dims = (((1,), (1,)), ((), ()))
        gate = lax.dot_general(mlp_in[...], w_all[0], dims, preferred_element_type=f32)
        up = lax.dot_general(mlp_in[...], w_all[1], dims, preferred_element_type=f32)
        active = (gate / (1.0 + jnp.exp(-gate)) * up).astype(bf16)
        for e in range(m):
            sums[t, e] = jnp.dot(
                active, w_all[2, :, e * width_q : (e + 1) * width_q], preferred_element_type=f32
            ).astype(bf16)
        for xx in range(nx):
            c_copy(t, xx).start()
        return carry

    lax.fori_loop(0, n, chunk, 0)

    def with_partner(bs, xx):
        c_copy(bs, xx).wait_recv()
        return sums[bs, mp_of(xx, c)].astype(f32) + c_buf[bs, xx].astype(f32)

    def b_copy(kind, zz, yy, xx):
        return remote(
            sums.at[seq_of(zz, yy), mp_of(xx, c)],
            b_buf.at[kind, zz],
            b_send.at[kind, zz],
            b_recv.at[kind, zz],
            dev_b,
        )

    def a_copy(zz):
        return remote(
            sums.at[seq_of(zz, ya), mp_of(xa, c)],
            a_buf.at[zz],
            a_send.at[zz],
            a_recv.at[zz],
            dev_a,
        )

    def zs_copy(dz, slot):
        zz = (z + dz) % nz
        return remote(
            sums.at[seq_of(zz, y), mp],
            z_buf.at[slot],
            zs_send.at[dz],
            zs_recv.at[slot],
            (seq_of(zz, y), mp),
        )

    order = list(range(1, nz)) + [0]
    for kind, (yy, xx) in ((1, (1 - y, 1 - x)), (0, (yb, xb))):
        for dz in order:
            zz = (z + dz) % nz
            bs = seq_of(zz, yy)
            sums[bs, mp_of(xx, c)] = with_partner(bs, xx).astype(bf16)
            b_copy(kind, zz, yy, xx).start()
    for dz in order:
        zz = (z + dz) % nz
        bs = seq_of(zz, ya)
        value = with_partner(bs, xa)
        b_copy(1, zz, yb, xb).wait_recv()
        sums[bs, mp_of(xa, c)] = (value + b_buf[1, zz].astype(f32)).astype(bf16)
        a_copy(zz).start()
    own = None
    for dz in order:
        zz = (z + dz) % nz
        bs = seq_of(zz, y)
        value = with_partner(bs, x)
        b_copy(0, zz, yb, xb).wait_recv()
        a_copy(zz).wait_recv()
        value = value + b_buf[0, zz].astype(f32) + a_buf[zz].astype(f32)
        if dz:
            sums[bs, mp] = value.astype(bf16)
            zs_copy(dz, z).start()
        else:
            own = value
    for dz in range(1, nz):
        slot = (z + dz) % nz
        zs_copy(dz, slot).wait_recv()
        own = own + z_buf[slot].astype(f32)
    out_ref[...] = (resid[s, mp].astype(f32) + own).astype(bf16)

    for d in range(1, n):
        @pl.when((s + d) % n > s)
        def _():
            kv_copy(d).wait_send()

        w_copy(d).wait_send()
    for j in range(n):
        @pl.when(j < s)
        def _():
            fw_copy(j, c).wait_send()
    for e in range(1, m):
        rs_copy(e).wait_send()
    for dz in range(nz):
        zz = (z + dz) % nz
        if dz:
            z_copy(dz).wait_send()
            zs_copy(dz, z).wait_send()
        ag_copy(0, seq_of(zz, y), mp, dev_a).wait_send()
        ag_copy(1, seq_of(zz, y), mp, dev_b).wait_send()
        ag_copy(1, seq_of(zz, ya), mp_of(xa, c), dev_b).wait_send()
        for yy, xx in ((y, x), (ya, xa), (yb, xb), (1 - y, 1 - x)):
            ag_copy(2, seq_of(zz, yy), mp_of(xx, c), dev_c).wait_send()
        b_copy(0, zz, yb, xb).wait_send()
        b_copy(1, zz, 1 - y, 1 - x).wait_send()
        a_copy(zz).wait_send()
    for t in range(n):
        for xx in range(nx):
            c_copy(t, xx).wait_send()


def run_layer(n, m, queries, kv_here, weights, o_weight, own_in, gain):
    tok, width_q = own_in.shape
    seqs_n, heads_here, tok_n, head_w = queries.shape
    width = m * width_q
    _, _, ff_rows, rows = weights.shape
    nz, nx = n // PAIR, m // PAIR
    dt = jnp.bfloat16
    dma = pltpu.SemaphoreType.DMA
    block = (tok, width_q)
    return pl.pallas_call(
        functools.partial(layer_kernel, n, m),
        out_shape=jax.ShapeDtypeStruct(block, dt),
        in_specs=[pl.BlockSpec(memory_space=pltpu.VMEM)] * 6,
        out_specs=pl.BlockSpec(memory_space=pltpu.VMEM),
        scratch_shapes=[
            pltpu.VMEM((2, n, seqs_n, tok_n, head_w), dt),
            pltpu.VMEM((3, ff_rows, width), dt),
            pltpu.VMEM((tok, heads_here * head_w), dt),
            pltpu.VMEM((m,) + block, dt),
            pltpu.VMEM((m,) + block, dt),
            pltpu.VMEM((n, m) + block, dt),
            pltpu.VMEM((tok, width), dt),
            pltpu.VMEM((n, m) + block, dt),
            pltpu.VMEM((n, nx) + block, dt),
            pltpu.VMEM((2, nz) + block, dt),
            pltpu.VMEM((nz,) + block, dt),
            pltpu.VMEM((nz,) + block, dt),
            dma((n,)),
            dma((n,)),
            dma((n,)),
            dma((n,)),
            dma((n,)),
            dma((n,)),
            dma((m,)),
            dma((m,)),
            dma((nz,)),
            dma((3, n, m)),
            dma((n, m)),
            dma((n, nx)),
            dma((n, nx)),
            dma((2, nz)),
            dma((2, nz)),
            dma((nz,)),
            dma((nz,)),
            dma((nz,)),
            dma((nz,)),
        ],
        compiler_params=pltpu.CompilerParams(
            collective_id=0, has_side_effects=True, vmem_limit_bytes=VMEM_BYTES
        ),
    )(queries, kv_here, weights, o_weight, own_in, gain)


def local_fast(
    hidden_in,
    attn_gain,
    q_weight,
    q_bias,
    k_weight,
    k_bias,
    v_weight,
    v_bias,
    o_weight,
    mlp_gain,
    gate_weight,
    up_weight,
    down_weight,
    lengths,
):
    seqs_n, tok_n, width = hidden_in.shape
    n = lax.axis_size("seq")
    m = lax.axis_size("mp")
    seq_rank = lax.axis_index("seq")
    mp_rank = lax.axis_index("mp")
    heads_here = q_weight.shape[1] // HEAD
    kv_index = mp_rank * heads_here // (HEADS // KV_HEADS)
    quarter = width // m
    flat_in = hidden_in.reshape(seqs_n * tok_n, width)
    weights = jnp.stack([gate_weight.T, up_weight.T, down_weight.T])
    weights = weights.reshape(3, n, gate_weight.shape[1] // n, gate_weight.shape[0])
    normed = rms_scale(flat_in, attn_gain)
    query_all = jnp.dot(normed, q_weight, preferred_element_type=jnp.float32) + q_bias
    key_cols = lax.dynamic_slice_in_dim(k_weight, kv_index * HEAD, HEAD, 1)
    value_cols = lax.dynamic_slice_in_dim(v_weight, kv_index * HEAD, HEAD, 1)
    key_shift = lax.dynamic_slice_in_dim(k_bias, kv_index * HEAD, HEAD, 0)
    value_shift = lax.dynamic_slice_in_dim(v_bias, kv_index * HEAD, HEAD, 0)
    key_all = jnp.dot(normed, key_cols, preferred_element_type=jnp.float32) + key_shift
    value_rows = (
        jnp.dot(normed, value_cols, preferred_element_type=jnp.float32) + value_shift
    ).astype(jnp.bfloat16)
    positions = seq_rank * tok_n + jnp.arange(tok_n, dtype=jnp.int32)
    rotated_q = rotate(
        query_all.reshape(seqs_n, tok_n, heads_here, HEAD).transpose(0, 2, 1, 3), positions
    ).astype(jnp.bfloat16)
    rotated_k = rotate(key_all.reshape(seqs_n, tok_n, HEAD), positions).astype(jnp.bfloat16)
    value_rows = value_rows.reshape(seqs_n, tok_n, HEAD)
    own_in = lax.dynamic_slice_in_dim(flat_in, mp_rank * quarter, quarter, 1)
    layer_part = run_layer(
        n,
        m,
        rotated_q,
        jnp.stack([rotated_k, value_rows]),
        weights,
        o_weight,
        own_in,
        mlp_gain[None, :],
    )
    in_share = own_in.astype(jnp.float32)
    out_share = layer_part.astype(jnp.float32)
    cross_part = jnp.sum(in_share * out_share, axis=-1).reshape(seqs_n, tok_n)
    out_part = jnp.sum(out_share * out_share, axis=-1).reshape(seqs_n, tok_n)
    cross, out_norm = lax.psum((cross_part, out_part), "mp")
    in_wide = flat_in.astype(jnp.float32)
    in_norm = jnp.sum(in_wide * in_wide, axis=-1).reshape(seqs_n, tok_n)
    cosine = cross / jnp.sqrt((in_norm + norm_eps) * (out_norm + norm_eps))
    valid = positions[None, :] < lengths[:, None]
    influence = jnp.where(valid, 1.0 - cosine, 0.0)
    seq_total = lax.psum(jnp.sum(influence, axis=1), "seq")
    score = seq_total / lengths.astype(jnp.float32)
    return (layer_part.reshape(seqs_n, tok_n, quarter), influence, score)


def fits_on_chip(n, m, hidden_in, q_weight, gate_weight):
    seqs_n, tok_n, width = hidden_in.shape
    heads_here = q_weight.shape[1] // HEAD
    ff_here, rows = gate_weight.shape[1], gate_weight.shape[0]
    shared_kv = (HEADS // KV_HEADS) % (PAIR * heads_here) == 0
    even = n % PAIR == 0 and m == PAIR * PAIR and ff_here % (16 * n) == 0
    tiled = rows % 128 == 0 and tok_n % 16 == 0 and (n * tok_n) % 128 == 0
    tiled = tiled and width % (128 * m) == 0
    held = n * seqs_n * tok_n * width * 2 * 3
    return shared_kv and even and tiled and held < VMEM_BYTES // 2


def body(*args):
    n, m = lax.axis_size("seq"), lax.axis_size("mp")
    if fits_on_chip(n, m, args[0], args[2], args[10]):
        return local_fast(*args)
    return local(*args)


def solution(mesh):
    placed = (
        P(None, "seq", None),
        P(),
        P(None, "mp"),
        P("mp"),
        P(),
        P(),
        P(),
        P(),
        P("mp", None),
        P(),
        P("seq", "mp"),
        P("seq", "mp"),
        P("seq", "mp"),
        P(),
    )
    return jax.shard_map(
        body,
        mesh=mesh,
        in_specs=placed,
        out_specs=(P(None, "seq", "mp"), P(None, "seq"), P()),
        check_vma=False,
    )
```

```python
import functools

import jax
import jax.numpy as jnp
from jax import lax
from jax.experimental import pallas as pl
from jax.experimental.pallas import tpu as pltpu
from jax.sharding import PartitionSpec as P

HEADS = 16
KV_HEADS = 2
HEAD = 128


rope_base = 1000000.0
norm_eps = 1e-06
masked_score = -1e30


def rms_scale(values, gain):
    widened = values.astype(jnp.float32)
    factor = lax.rsqrt(jnp.mean(widened * widened, axis=-1, keepdims=True) + norm_eps)
    return (widened * factor * gain).astype(jnp.bfloat16)


def rotate(values, positions):
    head_width = values.shape[-1]
    half_width = head_width // 2
    inv_freq = rope_base ** (-(jnp.arange(half_width, dtype=jnp.float32) * 2.0) / head_width)
    angles = positions.astype(jnp.float32)[:, None] * inv_freq[None, :]
    angles = jnp.concatenate([angles, angles], axis=-1)
    first_part = values[..., :half_width]
    second_part = values[..., half_width:]
    turned = jnp.concatenate([-second_part, first_part], axis=-1)
    return values * jnp.cos(angles) + turned * jnp.sin(angles)


def attend_update(state, queries, first_pos, key_piece, value_piece):
    run_max, run_sum, run_acc = state
    score_scale = queries.shape[-1] ** (-0.5)
    query_pos = first_pos + jnp.arange(queries.shape[2], dtype=jnp.int32)
    key_pos = jnp.arange(key_piece.shape[1], dtype=jnp.int32)
    scores = (
        jnp.einsum("shqd,skd->shqk", queries, key_piece, preferred_element_type=jnp.float32)
        * score_scale
    )
    allowed = key_pos[None, :] <= query_pos[:, None]
    scores = jnp.where(allowed, scores, masked_score)
    new_max = jnp.maximum(run_max, jnp.max(scores, axis=-1))
    weights = jnp.where(allowed, jnp.exp(scores - new_max[..., None]), 0.0)
    new_sum = jnp.sum(weights, axis=-1)
    mixed = jnp.einsum(
        "shqk,skd->shqd",
        weights.astype(jnp.bfloat16),
        value_piece,
        preferred_element_type=jnp.float32,
    )
    return (new_max, new_sum, mixed)


def local(
    hidden_in,
    attn_gain,
    q_weight,
    q_bias,
    k_weight,
    k_bias,
    v_weight,
    v_bias,
    o_weight,
    mlp_gain,
    gate_weight,
    up_weight,
    down_weight,
    lengths,
):
    seqs_n, tok_n, width = hidden_in.shape
    seq_rank = lax.axis_index("seq")
    mp_devices = lax.axis_size("mp")
    mp_rank = lax.axis_index("mp")
    heads_here = q_weight.shape[1] // HEAD
    group_size = HEADS // KV_HEADS
    kv_index = mp_rank * heads_here // group_size
    flat_in = hidden_in.reshape(seqs_n * tok_n, width)
    normed = rms_scale(flat_in, attn_gain)
    query_all = jnp.dot(normed, q_weight, preferred_element_type=jnp.float32) + q_bias
    key_cols = lax.dynamic_slice_in_dim(k_weight, kv_index * HEAD, HEAD, 1)
    value_cols = lax.dynamic_slice_in_dim(v_weight, kv_index * HEAD, HEAD, 1)
    key_shift = lax.dynamic_slice_in_dim(k_bias, kv_index * HEAD, HEAD, 0)
    value_shift = lax.dynamic_slice_in_dim(v_bias, kv_index * HEAD, HEAD, 0)
    key_all = jnp.dot(normed, key_cols, preferred_element_type=jnp.float32) + key_shift
    value_rows = (
        jnp.dot(normed, value_cols, preferred_element_type=jnp.float32) + value_shift
    ).astype(jnp.bfloat16)
    positions = seq_rank * tok_n + jnp.arange(tok_n, dtype=jnp.int32)
    rotated_q = rotate(
        query_all.reshape(seqs_n, tok_n, heads_here, HEAD).transpose(0, 2, 1, 3), positions
    ).astype(jnp.bfloat16)
    rotated_k = rotate(key_all.reshape(seqs_n, tok_n, HEAD), positions).astype(jnp.bfloat16)
    value_rows = value_rows.reshape(seqs_n, tok_n, HEAD)
    query_sets = ((rotated_q, seq_rank * tok_n),)
    initial = tuple(
        (
            (
                jnp.full(entry[0].shape[:3], masked_score, jnp.float32),
                jnp.zeros(entry[0].shape[:3], jnp.float32),
                jnp.zeros(entry[0].shape, jnp.float32),
            )
            for entry in query_sets
        )
    )
    key_start = jnp.int32(0)
    key_piece = lax.all_gather(rotated_k, "seq", axis=1, tiled=True)
    value_piece = lax.all_gather(value_rows, "seq", axis=1, tiled=True)
    updated = []
    for state, query_entry in zip(initial, query_sets):
        queries, first_pos = query_entry
        last_pos = first_pos + queries.shape[2] - 1

        def run_update(current):
            return attend_update(current, queries, first_pos, key_piece, value_piece)

        def keep_state(current):
            return current

        updated.append(lax.cond(key_start <= last_pos, run_update, keep_state, state))
    results = tuple(updated)
    finished = [(entry[2] / entry[1][..., None]).astype(jnp.bfloat16) for entry in results]
    attn = finished[0]
    attn = attn.transpose(0, 2, 1, 3).reshape(seqs_n * tok_n, heads_here * HEAD)
    projected = jnp.dot(attn, o_weight, preferred_element_type=jnp.float32)
    quarter = width // mp_devices
    own_in = lax.dynamic_slice_in_dim(flat_in, mp_rank * quarter, quarter, 1)
    summed = lax.psum(projected.astype(jnp.bfloat16), "mp").astype(jnp.float32)
    residual = (flat_in.astype(jnp.float32) + summed).astype(jnp.bfloat16)
    resid_part = lax.dynamic_slice_in_dim(residual, mp_rank * quarter, quarter, 1)
    mlp_in = rms_scale(residual, mlp_gain)
    gate_sum = jnp.dot(
        mlp_in,
        lax.all_gather(gate_weight, "seq", axis=0, tiled=True),
        preferred_element_type=jnp.float32,
    )
    up_sum = jnp.dot(
        mlp_in,
        lax.all_gather(up_weight, "seq", axis=0, tiled=True),
        preferred_element_type=jnp.float32,
    )
    activated = (jax.nn.silu(gate_sum) * up_sum).astype(jnp.bfloat16)
    down_part = lax.dot_general(
        activated,
        lax.all_gather(down_weight, "seq", axis=0, tiled=True),
        (((1,), (1,)), ((), ())),
        preferred_element_type=jnp.float32,
    )
    mlp_share = lax.psum_scatter(
        down_part.astype(jnp.bfloat16), "mp", scatter_dimension=1, tiled=True
    ).astype(jnp.float32)
    layer_part = (resid_part.astype(jnp.float32) + mlp_share).astype(jnp.bfloat16)
    in_share = own_in.astype(jnp.float32)
    out_share = layer_part.astype(jnp.float32)
    cross_part = jnp.sum(in_share * out_share, axis=-1).reshape(seqs_n, tok_n)
    out_part = jnp.sum(out_share * out_share, axis=-1).reshape(seqs_n, tok_n)
    cross, out_norm = lax.psum((cross_part, out_part), "mp")
    in_wide = flat_in.astype(jnp.float32)
    in_norm = jnp.sum(in_wide * in_wide, axis=-1).reshape(seqs_n, tok_n)
    cosine = cross / jnp.sqrt((in_norm + norm_eps) * (out_norm + norm_eps))
    valid = positions[None, :] < lengths[:, None]
    influence = jnp.where(valid, 1.0 - cosine, 0.0)
    seq_total = lax.psum(jnp.sum(influence, axis=1), "seq")
    score = seq_total / lengths.astype(jnp.float32)
    return (layer_part.reshape(seqs_n, tok_n, quarter), influence, score)


MESH = pl.DeviceIdType.MESH
PAIR = 2
VMEM_BYTES = 60 * 1024 * 1024


def layer_kernel(
    n,
    m,
    x_ref,
    ag_ref,
    qw_ref,
    qb_ref,
    kw_ref,
    kb_ref,
    vw_ref,
    vb_ref,
    cos_ref,
    sin_ref,
    w_ref,
    o_ref,
    g_ref,
    len_ref,
    out_ref,
    inf_ref,
    tot_ref,
    q_all,
    stat,
    tot_all,
    kv_all,
    w_all,
    attn,
    part,
    rs_buf,
    resid,
    mlp_in,
    sums,
    c_buf,
    b_buf,
    a_buf,
    z_buf,
    kv_send,
    kv_recv,
    fw_send,
    fw_recv,
    w_send,
    w_recv,
    rs_send,
    rs_recv,
    zg_send,
    ag_send,
    ag_recv,
    c_send,
    c_recv,
    b_send,
    b_recv,
    a_send,
    a_recv,
    zs_send,
    zs_recv,
    st_send,
    st_recv,
    tt_send,
    tt_recv,
):
    f32, bf16 = jnp.float32, jnp.bfloat16
    s = lax.axis_index("seq")
    mp = lax.axis_index("mp")
    nz = n // PAIR
    nx = m // PAIR
    z, y = s // PAIR, s % PAIR
    x, c = mp // PAIR, mp % PAIR
    tok, width = x_ref.shape
    width_q = width // m
    tok_n, head_w = cos_ref.shape
    seqs_n = tok // tok_n
    heads_here = qw_ref.shape[1] // head_w
    quarter = pl.ds(pl.multiple_of(mp * width_q, width_q), width_q)
    kv_at = mp * heads_here // (HEADS // KV_HEADS)
    kv_cols = pl.ds(pl.multiple_of(kv_at * head_w, head_w), head_w)
    rows = w_ref.shape[3]

    def seq_of(zz, yy):
        return zz * PAIR + yy

    def mp_of(xx, cc):
        return xx * PAIR + cc

    ya, xa = y + (1 - c) * (1 - 2 * y), x + c * (1 - 2 * x)
    yb, xb = y + c * (1 - 2 * y), x + (1 - c) * (1 - 2 * x)
    dev_a = (seq_of(z, ya), mp_of(xa, c))
    dev_b = (seq_of(z, yb), mp_of(xb, c))
    dev_c = (s, mp_of(x, 1 - c))

    def remote(source, target, sent, arrived, device):
        return pltpu.make_async_remote_copy(
            src_ref=source,
            dst_ref=target,
            send_sem=sent,
            recv_sem=arrived,
            device_id=device,
            device_id_type=MESH,
        )

    barrier = pltpu.get_barrier_semaphore()
    for d in range(1, n):
        pl.semaphore_signal(barrier, inc=1, device_id=((s + d) % n, mp), device_id_type=MESH)
    for d in range(1, m):
        pl.semaphore_signal(barrier, inc=1, device_id=(s, (mp + d) % m), device_id_type=MESH)
    pl.semaphore_wait(barrier, n - 1 + m - 1)

    def kv_copy(d):
        return remote(
            kv_all.at[c, s], kv_all.at[c, s], kv_send.at[d], kv_recv.at[s], ((s + d) % n, mp)
        )

    def w_copy(d):
        peer = (s + d) % n
        here = pl.ds(pl.multiple_of(s * rows, rows), rows)
        return remote(
            w_ref.at[:, peer], w_all.at[:, :, here], w_send.at[d], w_recv.at[s], (peer, mp)
        )

    wide = x_ref[...].astype(f32)
    factor = lax.rsqrt(jnp.mean(wide * wide, axis=-1, keepdims=True) + norm_eps)
    mlp_in[...] = (wide * factor * ag_ref[...]).astype(bf16)

    def turn(values):
        return values * cos_ref[...] + pltpu.roll(values, head_w // 2, 1) * sin_ref[...]

    keys = jnp.dot(mlp_in[...], kw_ref[:, kv_cols], preferred_element_type=f32)
    keys = keys + kb_ref[:, kv_cols]
    vals = jnp.dot(mlp_in[...], vw_ref[:, kv_cols], preferred_element_type=f32)
    vals = vals + vb_ref[:, kv_cols]
    for i in range(seqs_n):
        span = slice(i * tok_n, (i + 1) * tok_n)
        kv_all[0, s, i] = turn(keys[span]).astype(bf16)
        kv_all[1, s, i] = vals[span].astype(bf16)

    for d in range(1, n):
        @pl.when((s + d) % n > s)
        def _():
            kv_copy(d).start()

    for d in range(1, n):
        w_copy(d).start()

    for h in range(heads_here):
        cols = slice(h * head_w, (h + 1) * head_w)
        query = jnp.dot(mlp_in[...], qw_ref[:, cols], preferred_element_type=f32)
        query = query + qb_ref[:, cols]
        for i in range(seqs_n):
            q_all[i, h] = turn(query[i * tok_n : (i + 1) * tok_n]).astype(bf16)

    w_all[:, :, pl.ds(pl.multiple_of(s * rows, rows), rows)] = w_ref[:, s]
    for j in range(n):
        @pl.when(j > s)
        def _():
            kv_all[0, j] = jnp.zeros(kv_all.shape[2:], bf16)
            kv_all[1, j] = jnp.zeros(kv_all.shape[2:], bf16)

    def fw_copy(j, cc):
        return remote(kv_all.at[cc, j], kv_all.at[cc, j], fw_send.at[j], fw_recv.at[j], dev_c)

    for j in range(n):
        @pl.when(j < s)
        def _():
            remote(
                kv_all.at[c, s], kv_all.at[c, j], kv_send.at[0], kv_recv.at[j], dev_c
            ).wait_recv()
            fw_copy(j, c).start()

    for j in range(n):
        @pl.when(j < s)
        def _():
            fw_copy(j, 1 - c).wait_recv()

    scale = head_w ** (-0.5)
    query_pos = s * tok_n + lax.broadcasted_iota(jnp.int32, (tok_n, n * tok_n), 0)
    key_pos = lax.broadcasted_iota(jnp.int32, (tok_n, n * tok_n), 1)
    allowed = key_pos <= query_pos
    for i in range(seqs_n):
        keys = kv_all[0, :, i].reshape(n * tok_n, head_w)
        vals = kv_all[1, :, i].reshape(n * tok_n, head_w)
        for h in range(heads_here):
            scores = lax.dot_general(
                q_all[i, h], keys, (((1,), (1,)), ((), ())), preferred_element_type=f32
            )
            scores = jnp.where(allowed, scores * scale, masked_score)
            top = jnp.max(scores, axis=-1, keepdims=True)
            weights = jnp.where(allowed, jnp.exp(scores - top), 0.0)
            total = jnp.sum(weights, axis=-1, keepdims=True)
            mixed = jnp.dot(weights.astype(bf16), vals, preferred_element_type=f32)
            attn[i * tok_n : (i + 1) * tok_n, h * head_w : (h + 1) * head_w] = (
                mixed / total
            ).astype(bf16)

    for e in range(m):
        part[e] = jnp.dot(
            attn[...], o_ref[:, e * width_q : (e + 1) * width_q], preferred_element_type=f32
        ).astype(bf16)

    def rs_copy(e):
        peer = (mp + e) % m
        return remote(part.at[peer], rs_buf.at[mp], rs_send.at[e], rs_recv.at[mp], (s, peer))

    for e in range(1, m):
        rs_copy(e).start()
    summed = part[mp].astype(f32)
    for e in range(1, m):
        peer = (mp + e) % m
        remote(
            part.at[peer], rs_buf.at[peer], rs_send.at[e], rs_recv.at[peer], (s, peer)
        ).wait_recv()
        summed = summed + rs_buf[peer].astype(f32)
    resid[s, mp] = (x_ref[:, quarter].astype(f32) + summed).astype(bf16)

    def ag_copy(kind, bs, bm, device):
        return remote(
            resid.at[bs, bm], resid.at[bs, bm], ag_send.at[kind, bs, bm], ag_recv.at[bs, bm], device
        )

    def ag_wait(bs, bm):
        ag_copy(0, bs, bm, dev_c).wait_recv()

    def z_copy(dz):
        return remote(
            resid.at[s, mp],
            resid.at[s, mp],
            zg_send.at[dz],
            ag_recv.at[s, mp],
            (seq_of((z + dz) % nz, y), mp),
        )

    for dz in range(1, nz):
        z_copy(dz).start()
    for dz in range(nz):
        bs, bm = seq_of((z + dz) % nz, y), mp
        if dz:
            ag_wait(bs, bm)
        ag_copy(0, bs, bm, dev_a).start()
        ag_copy(1, bs, bm, dev_b).start()
        ag_copy(2, bs, bm, dev_c).start()
    for dz in range(nz):
        bs, bm = seq_of((z + dz) % nz, ya), mp_of(xa, c)
        ag_wait(bs, bm)
        ag_copy(1, bs, bm, dev_b).start()
        ag_copy(2, bs, bm, dev_c).start()
    for dz in range(nz):
        for yy, xx in ((yb, xb), (1 - y, 1 - x)):
            bs, bm = seq_of((z + dz) % nz, yy), mp_of(xx, c)
            ag_wait(bs, bm)
            ag_copy(2, bs, bm, dev_c).start()

    for d in range(1, n):
        peer = (s + d) % n
        here = pl.ds(pl.multiple_of(peer * rows, rows), rows)
        remote(
            w_ref.at[:, peer], w_all.at[:, :, here], w_send.at[d], w_recv.at[peer], (peer, mp)
        ).wait_recv()

    def c_copy(t, xx):
        return remote(
            sums.at[t, mp_of(xx, 1 - c)],
            c_buf.at[t, xx],
            c_send.at[t, xx],
            c_recv.at[t, xx],
            dev_c,
        )

    def chunk(t, carry):
        for xx in range(nx):
            ag_wait(t, mp_of(xx, 1 - c))
        total = jnp.zeros((tok, 1), f32)
        for e in range(m):
            piece = resid[t, e].astype(f32)
            total = total + jnp.sum(piece * piece, axis=-1, keepdims=True)
        factor = lax.rsqrt(total / (m * width_q) + norm_eps)
        for e in range(m):
            cols = slice(e * width_q, (e + 1) * width_q)
            mlp_in[:, cols] = (resid[t, e].astype(f32) * factor * g_ref[:, cols]).astype(bf16)
        dims = (((1,), (1,)), ((), ()))
        gate = lax.dot_general(mlp_in[...], w_all[0], dims, preferred_element_type=f32)
        up = lax.dot_general(mlp_in[...], w_all[1], dims, preferred_element_type=f32)
        active = (gate / (1.0 + jnp.exp(-gate)) * up).astype(bf16)
        for e in range(m):
            sums[t, e] = jnp.dot(
                active, w_all[2, :, e * width_q : (e + 1) * width_q], preferred_element_type=f32
            ).astype(bf16)
        for xx in range(nx):
            c_copy(t, xx).start()
        return carry

    lax.fori_loop(0, n, chunk, 0)

    def with_partner(bs, xx):
        c_copy(bs, xx).wait_recv()
        return sums[bs, mp_of(xx, c)].astype(f32) + c_buf[bs, xx].astype(f32)

    def b_copy(kind, zz, yy, xx):
        return remote(
            sums.at[seq_of(zz, yy), mp_of(xx, c)],
            b_buf.at[kind, zz],
            b_send.at[kind, zz],
            b_recv.at[kind, zz],
            dev_b,
        )

    def a_copy(zz):
        return remote(
            sums.at[seq_of(zz, ya), mp_of(xa, c)],
            a_buf.at[zz],
            a_send.at[zz],
            a_recv.at[zz],
            dev_a,
        )

    def zs_copy(dz, slot):
        zz = (z + dz) % nz
        return remote(
            sums.at[seq_of(zz, y), mp],
            z_buf.at[slot],
            zs_send.at[dz],
            zs_recv.at[slot],
            (seq_of(zz, y), mp),
        )

    order = list(range(1, nz)) + [0]
    for kind, (yy, xx) in ((1, (1 - y, 1 - x)), (0, (yb, xb))):
        for dz in order:
            zz = (z + dz) % nz
            bs = seq_of(zz, yy)
            sums[bs, mp_of(xx, c)] = with_partner(bs, xx).astype(bf16)
            b_copy(kind, zz, yy, xx).start()
    for dz in order:
        zz = (z + dz) % nz
        bs = seq_of(zz, ya)
        value = with_partner(bs, xa)
        b_copy(1, zz, yb, xb).wait_recv()
        sums[bs, mp_of(xa, c)] = (value + b_buf[1, zz].astype(f32)).astype(bf16)
        a_copy(zz).start()
    own = None
    for dz in order:
        zz = (z + dz) % nz
        bs = seq_of(zz, y)
        value = with_partner(bs, x)
        b_copy(0, zz, yb, xb).wait_recv()
        a_copy(zz).wait_recv()
        value = value + b_buf[0, zz].astype(f32) + a_buf[zz].astype(f32)
        if dz:
            sums[bs, mp] = value.astype(bf16)
            zs_copy(dz, z).start()
        else:
            own = value
    for dz in range(1, nz):
        slot = (z + dz) % nz
        zs_copy(dz, slot).wait_recv()
        own = own + z_buf[slot].astype(f32)
    layer_part = (resid[s, mp].astype(f32) + own).astype(bf16)
    out_ref[...] = layer_part
    share_out = layer_part.astype(f32)
    share_in = x_ref[:, quarter].astype(f32)
    lane = lax.broadcasted_iota(jnp.int32, (tok, 128), 1)
    cross = jnp.sum(share_in * share_out, axis=-1, keepdims=True)
    norm_out = jnp.sum(share_out * share_out, axis=-1, keepdims=True)
    norm_in = jnp.sum(share_in * share_in, axis=-1, keepdims=True)
    packed = jnp.where(lane == 0, cross, jnp.where(lane == 1, norm_out, norm_in))
    stat[mp] = packed.T[:8]

    def st_copy(e):
        return remote(
            stat.at[mp], stat.at[mp], st_send.at[e], st_recv.at[mp], (s, (mp + e) % m)
        )

    for e in range(1, m):
        st_copy(e).start()
    for e in range(1, m):
        peer = (mp + e) % m
        remote(stat.at[mp], stat.at[peer], st_send.at[e], st_recv.at[peer], (s, peer)).wait_recv()
    full = stat[0]
    for e in range(1, m):
        full = full + stat[e]
    cosine = full[0:1] / jnp.sqrt((full[2:3] + norm_eps) * (full[1:2] + norm_eps))
    places = s * tok_n + lax.broadcasted_iota(jnp.int32, (1, tok_n), 1)
    for i in range(seqs_n):
        valid = places < len_ref[i : i + 1]
        influence = jnp.where(valid, 1.0 - cosine[:, i * tok_n : (i + 1) * tok_n], 0.0)
        inf_ref[i : i + 1] = influence
        subtotal = jnp.sum(influence, axis=-1, keepdims=True)
        tot_all[s, i : i + 1] = jnp.broadcast_to(subtotal, (1, 128))

    def tt_copy(d):
        return remote(
            tot_all.at[s], tot_all.at[s], tt_send.at[d], tt_recv.at[s], ((s + d) % n, mp)
        )

    for d in range(1, n):
        tt_copy(d).start()
    for d in range(1, n):
        peer = (s + d) % n
        remote(
            tot_all.at[s], tot_all.at[peer], tt_send.at[d], tt_recv.at[peer], (peer, mp)
        ).wait_recv()
    whole = tot_all[0]
    for j in range(1, n):
        whole = whole + tot_all[j]
    tot_ref[...] = whole
    for e in range(1, m):
        st_copy(e).wait_send()
    for d in range(1, n):
        tt_copy(d).wait_send()

    for d in range(1, n):
        @pl.when((s + d) % n > s)
        def _():
            kv_copy(d).wait_send()

        w_copy(d).wait_send()
    for j in range(n):
        @pl.when(j < s)
        def _():
            fw_copy(j, c).wait_send()
    for e in range(1, m):
        rs_copy(e).wait_send()
    for dz in range(nz):
        zz = (z + dz) % nz
        if dz:
            z_copy(dz).wait_send()
            zs_copy(dz, z).wait_send()
        ag_copy(0, seq_of(zz, y), mp, dev_a).wait_send()
        ag_copy(1, seq_of(zz, y), mp, dev_b).wait_send()
        ag_copy(1, seq_of(zz, ya), mp_of(xa, c), dev_b).wait_send()
        for yy, xx in ((y, x), (ya, xa), (yb, xb), (1 - y, 1 - x)):
            ag_copy(2, seq_of(zz, yy), mp_of(xx, c), dev_c).wait_send()
        b_copy(0, zz, yb, xb).wait_send()
        b_copy(1, zz, 1 - y, 1 - x).wait_send()
        a_copy(zz).wait_send()
    for t in range(n):
        for xx in range(nx):
            c_copy(t, xx).wait_send()


def run_layer(n, m, seqs_n, *operands):
    tok, width = operands[0].shape
    tok_n, head_w = operands[8].shape
    heads_here = operands[2].shape[1] // head_w
    ff_rows = operands[10].shape[2]
    nz, nx = n // PAIR, m // PAIR
    dt = jnp.bfloat16
    dma = pltpu.SemaphoreType.DMA
    block = (tok, width // m)
    vmem = pl.BlockSpec(memory_space=pltpu.VMEM)
    return pl.pallas_call(
        functools.partial(layer_kernel, n, m),
        out_shape=(
            jax.ShapeDtypeStruct(block, dt),
            jax.ShapeDtypeStruct((seqs_n, tok_n), jnp.float32),
            jax.ShapeDtypeStruct((seqs_n, 128), jnp.float32),
        ),
        in_specs=[vmem] * len(operands),
        out_specs=(vmem, vmem, vmem),
        scratch_shapes=[
            pltpu.VMEM((seqs_n, heads_here, tok_n, head_w), dt),
            pltpu.VMEM((m, 8, tok), jnp.float32),
            pltpu.VMEM((n, seqs_n, 128), jnp.float32),
            pltpu.VMEM((2, n, seqs_n, tok_n, head_w), dt),
            pltpu.VMEM((3, ff_rows, width), dt),
            pltpu.VMEM((tok, heads_here * head_w), dt),
            pltpu.VMEM((m,) + block, dt),
            pltpu.VMEM((m,) + block, dt),
            pltpu.VMEM((n, m) + block, dt),
            pltpu.VMEM((tok, width), dt),
            pltpu.VMEM((n, m) + block, dt),
            pltpu.VMEM((n, nx) + block, dt),
            pltpu.VMEM((2, nz) + block, dt),
            pltpu.VMEM((nz,) + block, dt),
            pltpu.VMEM((nz,) + block, dt),
            dma((n,)),
            dma((n,)),
            dma((n,)),
            dma((n,)),
            dma((n,)),
            dma((n,)),
            dma((m,)),
            dma((m,)),
            dma((nz,)),
            dma((3, n, m)),
            dma((n, m)),
            dma((n, nx)),
            dma((n, nx)),
            dma((2, nz)),
            dma((2, nz)),
            dma((nz,)),
            dma((nz,)),
            dma((nz,)),
            dma((nz,)),
            dma((m,)),
            dma((m,)),
            dma((n,)),
            dma((n,)),
        ],
        compiler_params=pltpu.CompilerParams(
            collective_id=0, has_side_effects=True, vmem_limit_bytes=VMEM_BYTES
        ),
    )(*operands)


def local_fast(
    hidden_in,
    attn_gain,
    q_weight,
    q_bias,
    k_weight,
    k_bias,
    v_weight,
    v_bias,
    o_weight,
    mlp_gain,
    gate_weight,
    up_weight,
    down_weight,
    lengths,
):
    seqs_n, tok_n, width = hidden_in.shape
    n = lax.axis_size("seq")
    m = lax.axis_size("mp")
    seq_rank = lax.axis_index("seq")
    flat_in = hidden_in.reshape(seqs_n * tok_n, width)
    weights = jnp.stack([gate_weight.T, up_weight.T, down_weight.T])
    weights = weights.reshape(3, n, gate_weight.shape[1] // n, gate_weight.shape[0])
    half = HEAD // 2
    inv_freq = rope_base ** (-(jnp.arange(half, dtype=jnp.float32) * 2.0) / HEAD)
    positions = seq_rank * tok_n + jnp.arange(tok_n, dtype=jnp.int32)
    angles = positions.astype(jnp.float32)[:, None] * inv_freq[None, :]
    sines = jnp.sin(angles)
    cosines = jnp.cos(angles)
    layer_part, influence, totals = run_layer(
        n,
        m,
        seqs_n,
        flat_in,
        attn_gain[None, :],
        q_weight,
        q_bias[None, :],
        k_weight,
        k_bias[None, :],
        v_weight,
        v_bias[None, :],
        jnp.concatenate([cosines, cosines], axis=-1),
        jnp.concatenate([-sines, sines], axis=-1),
        weights,
        o_weight,
        mlp_gain[None, :],
        jnp.broadcast_to(lengths[:, None], (seqs_n, tok_n)),
    )
    score = totals[:, 0] / lengths.astype(jnp.float32)
    return (layer_part.reshape(seqs_n, tok_n, width // m), influence, score)


def fits_on_chip(n, m, hidden_in, q_weight, gate_weight):
    seqs_n, tok_n, width = hidden_in.shape
    heads_here = q_weight.shape[1] // HEAD
    ff_here, rows = gate_weight.shape[1], gate_weight.shape[0]
    shared_kv = (HEADS // KV_HEADS) % (PAIR * heads_here) == 0
    even = n % PAIR == 0 and m == PAIR * PAIR and ff_here % (16 * n) == 0
    tiled = rows % 128 == 0 and tok_n % 128 == 0
    tiled = tiled and width % (128 * m) == 0
    held = n * seqs_n * tok_n * width * 2 * 3
    return shared_kv and even and tiled and held < VMEM_BYTES // 2


def body(*args):
    n, m = lax.axis_size("seq"), lax.axis_size("mp")
    if fits_on_chip(n, m, args[0], args[2], args[10]):
        return local_fast(*args)
    return local(*args)


def solution(mesh):
    placed = (
        P(None, "seq", None),
        P(),
        P(None, "mp"),
        P("mp"),
        P(),
        P(),
        P(),
        P(),
        P("mp", None),
        P(),
        P("seq", "mp"),
        P("seq", "mp"),
        P("seq", "mp"),
        P(),
    )
    return jax.shard_map(
        body,
        mesh=mesh,
        in_specs=placed,
        out_specs=(P(None, "seq", "mp"), P(None, "seq"), P()),
        check_vma=False,
    )
```

```python
import functools

import jax
import jax.numpy as jnp
from jax import lax
from jax.experimental import pallas as pl
from jax.experimental.pallas import tpu as pltpu
from jax.sharding import PartitionSpec as P

HEADS = 16
KV_HEADS = 2
HEAD = 128


rope_base = 1000000.0
norm_eps = 1e-06
masked_score = -1e30


def rms_scale(values, gain):
    widened = values.astype(jnp.float32)
    factor = lax.rsqrt(jnp.mean(widened * widened, axis=-1, keepdims=True) + norm_eps)
    return (widened * factor * gain).astype(jnp.bfloat16)


def rotate(values, positions):
    head_width = values.shape[-1]
    half_width = head_width // 2
    inv_freq = rope_base ** (-(jnp.arange(half_width, dtype=jnp.float32) * 2.0) / head_width)
    angles = positions.astype(jnp.float32)[:, None] * inv_freq[None, :]
    angles = jnp.concatenate([angles, angles], axis=-1)
    first_part = values[..., :half_width]
    second_part = values[..., half_width:]
    turned = jnp.concatenate([-second_part, first_part], axis=-1)
    return values * jnp.cos(angles) + turned * jnp.sin(angles)


def attend_update(state, queries, first_pos, key_piece, value_piece):
    run_max, run_sum, run_acc = state
    score_scale = queries.shape[-1] ** (-0.5)
    query_pos = first_pos + jnp.arange(queries.shape[2], dtype=jnp.int32)
    key_pos = jnp.arange(key_piece.shape[1], dtype=jnp.int32)
    scores = (
        jnp.einsum("shqd,skd->shqk", queries, key_piece, preferred_element_type=jnp.float32)
        * score_scale
    )
    allowed = key_pos[None, :] <= query_pos[:, None]
    scores = jnp.where(allowed, scores, masked_score)
    new_max = jnp.maximum(run_max, jnp.max(scores, axis=-1))
    weights = jnp.where(allowed, jnp.exp(scores - new_max[..., None]), 0.0)
    new_sum = jnp.sum(weights, axis=-1)
    mixed = jnp.einsum(
        "shqk,skd->shqd",
        weights.astype(jnp.bfloat16),
        value_piece,
        preferred_element_type=jnp.float32,
    )
    return (new_max, new_sum, mixed)


def local(
    hidden_in,
    attn_gain,
    q_weight,
    q_bias,
    k_weight,
    k_bias,
    v_weight,
    v_bias,
    o_weight,
    mlp_gain,
    gate_weight,
    up_weight,
    down_weight,
    lengths,
):
    seqs_n, tok_n, width = hidden_in.shape
    seq_rank = lax.axis_index("seq")
    mp_devices = lax.axis_size("mp")
    mp_rank = lax.axis_index("mp")
    heads_here = q_weight.shape[1] // HEAD
    group_size = HEADS // KV_HEADS
    kv_index = mp_rank * heads_here // group_size
    flat_in = hidden_in.reshape(seqs_n * tok_n, width)
    normed = rms_scale(flat_in, attn_gain)
    query_all = jnp.dot(normed, q_weight, preferred_element_type=jnp.float32) + q_bias
    key_cols = lax.dynamic_slice_in_dim(k_weight, kv_index * HEAD, HEAD, 1)
    value_cols = lax.dynamic_slice_in_dim(v_weight, kv_index * HEAD, HEAD, 1)
    key_shift = lax.dynamic_slice_in_dim(k_bias, kv_index * HEAD, HEAD, 0)
    value_shift = lax.dynamic_slice_in_dim(v_bias, kv_index * HEAD, HEAD, 0)
    key_all = jnp.dot(normed, key_cols, preferred_element_type=jnp.float32) + key_shift
    value_rows = (
        jnp.dot(normed, value_cols, preferred_element_type=jnp.float32) + value_shift
    ).astype(jnp.bfloat16)
    positions = seq_rank * tok_n + jnp.arange(tok_n, dtype=jnp.int32)
    rotated_q = rotate(
        query_all.reshape(seqs_n, tok_n, heads_here, HEAD).transpose(0, 2, 1, 3), positions
    ).astype(jnp.bfloat16)
    rotated_k = rotate(key_all.reshape(seqs_n, tok_n, HEAD), positions).astype(jnp.bfloat16)
    value_rows = value_rows.reshape(seqs_n, tok_n, HEAD)
    query_sets = ((rotated_q, seq_rank * tok_n),)
    initial = tuple(
        (
            (
                jnp.full(entry[0].shape[:3], masked_score, jnp.float32),
                jnp.zeros(entry[0].shape[:3], jnp.float32),
                jnp.zeros(entry[0].shape, jnp.float32),
            )
            for entry in query_sets
        )
    )
    key_start = jnp.int32(0)
    key_piece = lax.all_gather(rotated_k, "seq", axis=1, tiled=True)
    value_piece = lax.all_gather(value_rows, "seq", axis=1, tiled=True)
    updated = []
    for state, query_entry in zip(initial, query_sets):
        queries, first_pos = query_entry
        last_pos = first_pos + queries.shape[2] - 1

        def run_update(current):
            return attend_update(current, queries, first_pos, key_piece, value_piece)

        def keep_state(current):
            return current

        updated.append(lax.cond(key_start <= last_pos, run_update, keep_state, state))
    results = tuple(updated)
    finished = [(entry[2] / entry[1][..., None]).astype(jnp.bfloat16) for entry in results]
    attn = finished[0]
    attn = attn.transpose(0, 2, 1, 3).reshape(seqs_n * tok_n, heads_here * HEAD)
    projected = jnp.dot(attn, o_weight, preferred_element_type=jnp.float32)
    quarter = width // mp_devices
    own_in = lax.dynamic_slice_in_dim(flat_in, mp_rank * quarter, quarter, 1)
    summed = lax.psum(projected.astype(jnp.bfloat16), "mp").astype(jnp.float32)
    residual = (flat_in.astype(jnp.float32) + summed).astype(jnp.bfloat16)
    resid_part = lax.dynamic_slice_in_dim(residual, mp_rank * quarter, quarter, 1)
    mlp_in = rms_scale(residual, mlp_gain)
    gate_sum = jnp.dot(
        mlp_in,
        lax.all_gather(gate_weight, "seq", axis=0, tiled=True),
        preferred_element_type=jnp.float32,
    )
    up_sum = jnp.dot(
        mlp_in,
        lax.all_gather(up_weight, "seq", axis=0, tiled=True),
        preferred_element_type=jnp.float32,
    )
    activated = (jax.nn.silu(gate_sum) * up_sum).astype(jnp.bfloat16)
    down_part = lax.dot_general(
        activated,
        lax.all_gather(down_weight, "seq", axis=0, tiled=True),
        (((1,), (1,)), ((), ())),
        preferred_element_type=jnp.float32,
    )
    mlp_share = lax.psum_scatter(
        down_part.astype(jnp.bfloat16), "mp", scatter_dimension=1, tiled=True
    ).astype(jnp.float32)
    layer_part = (resid_part.astype(jnp.float32) + mlp_share).astype(jnp.bfloat16)
    in_share = own_in.astype(jnp.float32)
    out_share = layer_part.astype(jnp.float32)
    cross_part = jnp.sum(in_share * out_share, axis=-1).reshape(seqs_n, tok_n)
    out_part = jnp.sum(out_share * out_share, axis=-1).reshape(seqs_n, tok_n)
    cross, out_norm = lax.psum((cross_part, out_part), "mp")
    in_wide = flat_in.astype(jnp.float32)
    in_norm = jnp.sum(in_wide * in_wide, axis=-1).reshape(seqs_n, tok_n)
    cosine = cross / jnp.sqrt((in_norm + norm_eps) * (out_norm + norm_eps))
    valid = positions[None, :] < lengths[:, None]
    influence = jnp.where(valid, 1.0 - cosine, 0.0)
    seq_total = lax.psum(jnp.sum(influence, axis=1), "seq")
    score = seq_total / lengths.astype(jnp.float32)
    return (layer_part.reshape(seqs_n, tok_n, quarter), influence, score)


MESH = pl.DeviceIdType.MESH
PAIR = 2
VMEM_BYTES = 60 * 1024 * 1024


def layer_kernel(
    n,
    m,
    x_ref,
    ag_ref,
    qw_ref,
    qb_ref,
    kw_ref,
    kb_ref,
    vw_ref,
    vb_ref,
    cos_ref,
    sin_ref,
    w_ref,
    o_ref,
    g_ref,
    len_ref,
    out_ref,
    inf_ref,
    tot_ref,
    q_all,
    stat,
    tot_all,
    kv_all,
    w_all,
    attn,
    part,
    rs_buf,
    resid,
    mlp_in,
    sums,
    c_buf,
    b_buf,
    a_buf,
    z_buf,
    kv_send,
    kv_recv,
    fw_send,
    fw_recv,
    w_send,
    w_recv,
    rs_send,
    rs_recv,
    zg_send,
    ag_send,
    ag_recv,
    c_send,
    c_recv,
    b_send,
    b_recv,
    a_send,
    a_recv,
    zs_send,
    zs_recv,
    st_send,
    st_recv,
    tt_send,
    tt_recv,
):
    f32, bf16 = jnp.float32, jnp.bfloat16
    s = lax.axis_index("seq")
    mp = lax.axis_index("mp")
    nz = n // PAIR
    nx = m // PAIR
    z, y = s // PAIR, s % PAIR
    x, c = mp // PAIR, mp % PAIR
    tok, width = x_ref.shape
    width_q = width // m
    tok_n, head_w = cos_ref.shape
    seqs_n = tok // tok_n
    heads_here = qw_ref.shape[1] // head_w
    quarter = pl.ds(pl.multiple_of(mp * width_q, width_q), width_q)
    kv_at = mp * heads_here // (HEADS // KV_HEADS)
    kv_cols = pl.ds(pl.multiple_of(kv_at * head_w, head_w), head_w)
    rows = w_ref.shape[3]

    def seq_of(zz, yy):
        return zz * PAIR + yy

    def mp_of(xx, cc):
        return xx * PAIR + cc

    ya, xa = y + (1 - c) * (1 - 2 * y), x + c * (1 - 2 * x)
    yb, xb = y + c * (1 - 2 * y), x + (1 - c) * (1 - 2 * x)
    dev_a = (seq_of(z, ya), mp_of(xa, c))
    dev_b = (seq_of(z, yb), mp_of(xb, c))
    dev_c = (s, mp_of(x, 1 - c))

    def remote(source, target, sent, arrived, device):
        return pltpu.make_async_remote_copy(
            src_ref=source,
            dst_ref=target,
            send_sem=sent,
            recv_sem=arrived,
            device_id=device,
            device_id_type=MESH,
        )

    barrier = pltpu.get_barrier_semaphore()
    for d in range(1, n):
        pl.semaphore_signal(barrier, inc=1, device_id=((s + d) % n, mp), device_id_type=MESH)
    for d in range(1, m):
        pl.semaphore_signal(barrier, inc=1, device_id=(s, (mp + d) % m), device_id_type=MESH)
    pl.semaphore_wait(barrier, n - 1 + m - 1)

    def kv_copy(d):
        return remote(
            kv_all.at[c, s], kv_all.at[c, s], kv_send.at[d], kv_recv.at[s], ((s + d) % n, mp)
        )

    def w_copy(d):
        peer = (s + d) % n
        here = pl.ds(pl.multiple_of(s * rows, rows), rows)
        return remote(
            w_ref.at[:, peer], w_all.at[:, :, here], w_send.at[d], w_recv.at[s], (peer, mp)
        )

    wide = x_ref[...].astype(f32)
    factor = lax.rsqrt(jnp.mean(wide * wide, axis=-1, keepdims=True) + norm_eps)
    mlp_in[...] = (wide * factor * ag_ref[...]).astype(bf16)

    def turn(values):
        return values * cos_ref[...] + pltpu.roll(values, head_w // 2, 1) * sin_ref[...]

    keys = jnp.dot(mlp_in[...], kw_ref[:, kv_cols], preferred_element_type=f32)
    keys = keys + kb_ref[:, kv_cols]
    vals = jnp.dot(mlp_in[...], vw_ref[:, kv_cols], preferred_element_type=f32)
    vals = vals + vb_ref[:, kv_cols]
    for i in range(seqs_n):
        span = slice(i * tok_n, (i + 1) * tok_n)
        kv_all[0, s, i] = turn(keys[span]).astype(bf16)
        kv_all[1, s, i] = vals[span].astype(bf16)

    for d in range(1, n):
        @pl.when((s + d) % n > s)
        def _():
            kv_copy(d).start()

    for d in range(1, n):
        w_copy(d).start()

    for h in range(heads_here):
        cols = slice(h * head_w, (h + 1) * head_w)
        query = jnp.dot(mlp_in[...], qw_ref[:, cols], preferred_element_type=f32)
        query = query + qb_ref[:, cols]
        for i in range(seqs_n):
            q_all[i, h] = turn(query[i * tok_n : (i + 1) * tok_n]).astype(bf16)

    w_all[:, :, pl.ds(pl.multiple_of(s * rows, rows), rows)] = w_ref[:, s]
    for j in range(n):
        @pl.when(j > s)
        def _():
            kv_all[0, j] = jnp.zeros(kv_all.shape[2:], bf16)
            kv_all[1, j] = jnp.zeros(kv_all.shape[2:], bf16)

    def fw_copy(j, cc):
        return remote(kv_all.at[cc, j], kv_all.at[cc, j], fw_send.at[j], fw_recv.at[j], dev_c)

    for j in range(n):
        @pl.when(j < s)
        def _():
            remote(
                kv_all.at[c, s], kv_all.at[c, j], kv_send.at[0], kv_recv.at[j], dev_c
            ).wait_recv()
            fw_copy(j, c).start()

    for j in range(n):
        @pl.when(j < s)
        def _():
            fw_copy(j, 1 - c).wait_recv()

    scale = head_w ** (-0.5)
    query_pos = s * tok_n + lax.broadcasted_iota(jnp.int32, (tok_n, n * tok_n), 0)
    key_pos = lax.broadcasted_iota(jnp.int32, (tok_n, n * tok_n), 1)
    allowed = key_pos <= query_pos
    for i in range(seqs_n):
        keys = kv_all[0, :, i].reshape(n * tok_n, head_w)
        vals = kv_all[1, :, i].reshape(n * tok_n, head_w)
        for h in range(heads_here):
            scores = lax.dot_general(
                q_all[i, h], keys, (((1,), (1,)), ((), ())), preferred_element_type=f32
            )
            scores = jnp.where(allowed, scores * scale, masked_score)
            top = jnp.max(scores, axis=-1, keepdims=True)
            weights = jnp.where(allowed, jnp.exp(scores - top), 0.0)
            total = jnp.sum(weights, axis=-1, keepdims=True)
            mixed = jnp.dot(weights.astype(bf16), vals, preferred_element_type=f32)
            attn[i * tok_n : (i + 1) * tok_n, h * head_w : (h + 1) * head_w] = (
                mixed / total
            ).astype(bf16)

    for e in range(m):
        part[e] = jnp.dot(
            attn[...], o_ref[:, e * width_q : (e + 1) * width_q], preferred_element_type=f32
        ).astype(bf16)

    def rs_copy(e):
        peer = (mp + e) % m
        return remote(part.at[peer], rs_buf.at[mp], rs_send.at[e], rs_recv.at[mp], (s, peer))

    for e in range(1, m):
        rs_copy(e).start()
    summed = part[mp].astype(f32)
    for e in range(1, m):
        peer = (mp + e) % m
        remote(
            part.at[peer], rs_buf.at[peer], rs_send.at[e], rs_recv.at[peer], (s, peer)
        ).wait_recv()
        summed = summed + rs_buf[peer].astype(f32)
    resid[s, mp] = (x_ref[:, quarter].astype(f32) + summed).astype(bf16)

    def ag_copy(kind, bs, bm, device):
        return remote(
            resid.at[bs, bm], resid.at[bs, bm], ag_send.at[kind, bs, bm], ag_recv.at[bs, bm], device
        )

    def ag_wait(bs, bm):
        ag_copy(0, bs, bm, dev_c).wait_recv()

    def z_copy(dz):
        return remote(
            resid.at[s, mp],
            resid.at[s, mp],
            zg_send.at[dz],
            ag_recv.at[s, mp],
            (seq_of((z + dz) % nz, y), mp),
        )

    for dz in range(1, nz):
        z_copy(dz).start()
    for dz in range(nz):
        bs, bm = seq_of((z + dz) % nz, y), mp
        if dz:
            ag_wait(bs, bm)
        ag_copy(0, bs, bm, dev_a).start()
        ag_copy(1, bs, bm, dev_b).start()
        ag_copy(2, bs, bm, dev_c).start()
    for dz in range(nz):
        bs, bm = seq_of((z + dz) % nz, ya), mp_of(xa, c)
        ag_wait(bs, bm)
        ag_copy(1, bs, bm, dev_b).start()
        ag_copy(2, bs, bm, dev_c).start()

    def pass_on(yy, xx):
        for dz in range(nz):
            bs, bm = seq_of((z + dz) % nz, yy), mp_of(xx, c)
            ag_wait(bs, bm)
            ag_copy(2, bs, bm, dev_c).start()

    pass_on(yb, xb)

    for d in range(1, n):
        peer = (s + d) % n
        here = pl.ds(pl.multiple_of(peer * rows, rows), rows)
        remote(
            w_ref.at[:, peer], w_all.at[:, :, here], w_send.at[d], w_recv.at[peer], (peer, mp)
        ).wait_recv()

    def c_copy(t, xx):
        return remote(
            sums.at[t, mp_of(xx, 1 - c)],
            c_buf.at[t, xx],
            c_send.at[t, xx],
            c_recv.at[t, xx],
            dev_c,
        )

    def chunk(t, carry):
        for xx in range(nx):
            ag_wait(t, mp_of(xx, 1 - c))
        total = jnp.zeros((tok, 1), f32)
        for e in range(m):
            piece = resid[t, e].astype(f32)
            total = total + jnp.sum(piece * piece, axis=-1, keepdims=True)
        factor = lax.rsqrt(total / (m * width_q) + norm_eps)
        for e in range(m):
            cols = slice(e * width_q, (e + 1) * width_q)
            mlp_in[:, cols] = (resid[t, e].astype(f32) * factor * g_ref[:, cols]).astype(bf16)
        dims = (((1,), (1,)), ((), ()))
        gate = lax.dot_general(mlp_in[...], w_all[0], dims, preferred_element_type=f32)
        up = lax.dot_general(mlp_in[...], w_all[1], dims, preferred_element_type=f32)
        active = (gate / (1.0 + jnp.exp(-gate)) * up).astype(bf16)
        for e in range(m):
            sums[t, e] = jnp.dot(
                active, w_all[2, :, e * width_q : (e + 1) * width_q], preferred_element_type=f32
            ).astype(bf16)
        for xx in range(nx):
            c_copy(t, xx).start()
        return carry

    def chunks(yy):
        def one(dz, carry):
            return chunk(seq_of((z + dz) % nz, yy), carry)

        lax.fori_loop(0, nz, one, 0)

    chunks(y)
    pass_on(1 - y, 1 - x)
    chunks(1 - y)

    def with_partner(bs, xx):
        c_copy(bs, xx).wait_recv()
        return sums[bs, mp_of(xx, c)].astype(f32) + c_buf[bs, xx].astype(f32)

    def b_copy(kind, zz, yy, xx):
        return remote(
            sums.at[seq_of(zz, yy), mp_of(xx, c)],
            b_buf.at[kind, zz],
            b_send.at[kind, zz],
            b_recv.at[kind, zz],
            dev_b,
        )

    def a_copy(zz):
        return remote(
            sums.at[seq_of(zz, ya), mp_of(xa, c)],
            a_buf.at[zz],
            a_send.at[zz],
            a_recv.at[zz],
            dev_a,
        )

    def zs_copy(dz, slot):
        zz = (z + dz) % nz
        return remote(
            sums.at[seq_of(zz, y), mp],
            z_buf.at[slot],
            zs_send.at[dz],
            zs_recv.at[slot],
            (seq_of(zz, y), mp),
        )

    order = list(range(1, nz)) + [0]
    for kind, (yy, xx) in ((1, (1 - y, 1 - x)), (0, (yb, xb))):
        for dz in order:
            zz = (z + dz) % nz
            bs = seq_of(zz, yy)
            sums[bs, mp_of(xx, c)] = with_partner(bs, xx).astype(bf16)
            b_copy(kind, zz, yy, xx).start()
    for dz in order:
        zz = (z + dz) % nz
        bs = seq_of(zz, ya)
        value = with_partner(bs, xa)
        b_copy(1, zz, yb, xb).wait_recv()
        sums[bs, mp_of(xa, c)] = (value + b_buf[1, zz].astype(f32)).astype(bf16)
        a_copy(zz).start()
    own = None
    for dz in order:
        zz = (z + dz) % nz
        bs = seq_of(zz, y)
        value = with_partner(bs, x)
        b_copy(0, zz, yb, xb).wait_recv()
        a_copy(zz).wait_recv()
        value = value + b_buf[0, zz].astype(f32) + a_buf[zz].astype(f32)
        if dz:
            sums[bs, mp] = value.astype(bf16)
            zs_copy(dz, z).start()
        else:
            own = value
    for dz in range(1, nz):
        slot = (z + dz) % nz
        zs_copy(dz, slot).wait_recv()
        own = own + z_buf[slot].astype(f32)
    layer_part = (resid[s, mp].astype(f32) + own).astype(bf16)
    out_ref[...] = layer_part
    share_out = layer_part.astype(f32)
    share_in = x_ref[:, quarter].astype(f32)
    lane = lax.broadcasted_iota(jnp.int32, (tok, 128), 1)
    cross = jnp.sum(share_in * share_out, axis=-1, keepdims=True)
    norm_out = jnp.sum(share_out * share_out, axis=-1, keepdims=True)
    norm_in = jnp.sum(share_in * share_in, axis=-1, keepdims=True)
    packed = jnp.where(lane == 0, cross, jnp.where(lane == 1, norm_out, norm_in))
    stat[mp] = packed.T[:8]

    def st_copy(e):
        return remote(
            stat.at[mp], stat.at[mp], st_send.at[e], st_recv.at[mp], (s, (mp + e) % m)
        )

    for e in range(1, m):
        st_copy(e).start()
    for e in range(1, m):
        peer = (mp + e) % m
        remote(stat.at[mp], stat.at[peer], st_send.at[e], st_recv.at[peer], (s, peer)).wait_recv()
    full = stat[0]
    for e in range(1, m):
        full = full + stat[e]
    cosine = full[0:1] / jnp.sqrt((full[2:3] + norm_eps) * (full[1:2] + norm_eps))
    places = s * tok_n + lax.broadcasted_iota(jnp.int32, (1, tok_n), 1)
    for i in range(seqs_n):
        valid = places < len_ref[i : i + 1]
        influence = jnp.where(valid, 1.0 - cosine[:, i * tok_n : (i + 1) * tok_n], 0.0)
        inf_ref[i : i + 1] = influence
        subtotal = jnp.sum(influence, axis=-1, keepdims=True)
        tot_all[s, i : i + 1] = jnp.broadcast_to(subtotal, (1, 128))

    def tt_copy(d):
        return remote(
            tot_all.at[s], tot_all.at[s], tt_send.at[d], tt_recv.at[s], ((s + d) % n, mp)
        )

    for d in range(1, n):
        tt_copy(d).start()
    for d in range(1, n):
        peer = (s + d) % n
        remote(
            tot_all.at[s], tot_all.at[peer], tt_send.at[d], tt_recv.at[peer], (peer, mp)
        ).wait_recv()
    whole = tot_all[0]
    for j in range(1, n):
        whole = whole + tot_all[j]
    tot_ref[...] = whole
    for e in range(1, m):
        st_copy(e).wait_send()
    for d in range(1, n):
        tt_copy(d).wait_send()

    for d in range(1, n):
        @pl.when((s + d) % n > s)
        def _():
            kv_copy(d).wait_send()

        w_copy(d).wait_send()
    for j in range(n):
        @pl.when(j < s)
        def _():
            fw_copy(j, c).wait_send()
    for e in range(1, m):
        rs_copy(e).wait_send()
    for dz in range(nz):
        zz = (z + dz) % nz
        if dz:
            z_copy(dz).wait_send()
            zs_copy(dz, z).wait_send()
        ag_copy(0, seq_of(zz, y), mp, dev_a).wait_send()
        ag_copy(1, seq_of(zz, y), mp, dev_b).wait_send()
        ag_copy(1, seq_of(zz, ya), mp_of(xa, c), dev_b).wait_send()
        for yy, xx in ((y, x), (ya, xa), (yb, xb), (1 - y, 1 - x)):
            ag_copy(2, seq_of(zz, yy), mp_of(xx, c), dev_c).wait_send()
        b_copy(0, zz, yb, xb).wait_send()
        b_copy(1, zz, 1 - y, 1 - x).wait_send()
        a_copy(zz).wait_send()
    for t in range(n):
        for xx in range(nx):
            c_copy(t, xx).wait_send()


def run_layer(n, m, seqs_n, *operands):
    tok, width = operands[0].shape
    tok_n, head_w = operands[8].shape
    heads_here = operands[2].shape[1] // head_w
    ff_rows = operands[10].shape[2]
    nz, nx = n // PAIR, m // PAIR
    dt = jnp.bfloat16
    dma = pltpu.SemaphoreType.DMA
    block = (tok, width // m)
    vmem = pl.BlockSpec(memory_space=pltpu.VMEM)
    return pl.pallas_call(
        functools.partial(layer_kernel, n, m),
        out_shape=(
            jax.ShapeDtypeStruct(block, dt),
            jax.ShapeDtypeStruct((seqs_n, tok_n), jnp.float32),
            jax.ShapeDtypeStruct((seqs_n, 128), jnp.float32),
        ),
        in_specs=[vmem] * len(operands),
        out_specs=(vmem, vmem, vmem),
        scratch_shapes=[
            pltpu.VMEM((seqs_n, heads_here, tok_n, head_w), dt),
            pltpu.VMEM((m, 8, tok), jnp.float32),
            pltpu.VMEM((n, seqs_n, 128), jnp.float32),
            pltpu.VMEM((2, n, seqs_n, tok_n, head_w), dt),
            pltpu.VMEM((3, ff_rows, width), dt),
            pltpu.VMEM((tok, heads_here * head_w), dt),
            pltpu.VMEM((m,) + block, dt),
            pltpu.VMEM((m,) + block, dt),
            pltpu.VMEM((n, m) + block, dt),
            pltpu.VMEM((tok, width), dt),
            pltpu.VMEM((n, m) + block, dt),
            pltpu.VMEM((n, nx) + block, dt),
            pltpu.VMEM((2, nz) + block, dt),
            pltpu.VMEM((nz,) + block, dt),
            pltpu.VMEM((nz,) + block, dt),
            dma((n,)),
            dma((n,)),
            dma((n,)),
            dma((n,)),
            dma((n,)),
            dma((n,)),
            dma((m,)),
            dma((m,)),
            dma((nz,)),
            dma((3, n, m)),
            dma((n, m)),
            dma((n, nx)),
            dma((n, nx)),
            dma((2, nz)),
            dma((2, nz)),
            dma((nz,)),
            dma((nz,)),
            dma((nz,)),
            dma((nz,)),
            dma((m,)),
            dma((m,)),
            dma((n,)),
            dma((n,)),
        ],
        compiler_params=pltpu.CompilerParams(
            collective_id=0, has_side_effects=True, vmem_limit_bytes=VMEM_BYTES
        ),
    )(*operands)


def local_fast(
    hidden_in,
    attn_gain,
    q_weight,
    q_bias,
    k_weight,
    k_bias,
    v_weight,
    v_bias,
    o_weight,
    mlp_gain,
    gate_weight,
    up_weight,
    down_weight,
    lengths,
):
    seqs_n, tok_n, width = hidden_in.shape
    n = lax.axis_size("seq")
    m = lax.axis_size("mp")
    seq_rank = lax.axis_index("seq")
    flat_in = hidden_in.reshape(seqs_n * tok_n, width)
    weights = jnp.stack([gate_weight.T, up_weight.T, down_weight.T])
    weights = weights.reshape(3, n, gate_weight.shape[1] // n, gate_weight.shape[0])
    half = HEAD // 2
    inv_freq = rope_base ** (-(jnp.arange(half, dtype=jnp.float32) * 2.0) / HEAD)
    positions = seq_rank * tok_n + jnp.arange(tok_n, dtype=jnp.int32)
    angles = positions.astype(jnp.float32)[:, None] * inv_freq[None, :]
    sines = jnp.sin(angles)
    cosines = jnp.cos(angles)
    layer_part, influence, totals = run_layer(
        n,
        m,
        seqs_n,
        flat_in,
        attn_gain[None, :],
        q_weight,
        q_bias[None, :],
        k_weight,
        k_bias[None, :],
        v_weight,
        v_bias[None, :],
        jnp.concatenate([cosines, cosines], axis=-1),
        jnp.concatenate([-sines, sines], axis=-1),
        weights,
        o_weight,
        mlp_gain[None, :],
        jnp.broadcast_to(lengths[:, None], (seqs_n, tok_n)),
    )
    score = totals[:, 0] / lengths.astype(jnp.float32)
    return (layer_part.reshape(seqs_n, tok_n, width // m), influence, score)


def fits_on_chip(n, m, hidden_in, q_weight, gate_weight):
    seqs_n, tok_n, width = hidden_in.shape
    heads_here = q_weight.shape[1] // HEAD
    ff_here, rows = gate_weight.shape[1], gate_weight.shape[0]
    shared_kv = (HEADS // KV_HEADS) % (PAIR * heads_here) == 0
    even = n % PAIR == 0 and m == PAIR * PAIR and ff_here % (16 * n) == 0
    tiled = rows % 128 == 0 and tok_n % 128 == 0
    tiled = tiled and width % (128 * m) == 0
    held = n * seqs_n * tok_n * width * 2 * 3
    return shared_kv and even and tiled and held < VMEM_BYTES // 2


def body(*args):
    n, m = lax.axis_size("seq"), lax.axis_size("mp")
    if fits_on_chip(n, m, args[0], args[2], args[10]):
        return local_fast(*args)
    return local(*args)


def solution(mesh):
    placed = (
        P(None, "seq", None),
        P(),
        P(None, "mp"),
        P("mp"),
        P(),
        P(),
        P(),
        P(),
        P("mp", None),
        P(),
        P("seq", "mp"),
        P("seq", "mp"),
        P("seq", "mp"),
        P(),
    )
    return jax.shard_map(
        body,
        mesh=mesh,
        in_specs=placed,
        out_specs=(P(None, "seq", "mp"), P(None, "seq"), P()),
        check_vma=False,
    )
```
